256 devices in a mesh: groups: 2 (over y), row: 16 (over z), col: 4 (over x), ksplit: 2 (over core).
Axes of the slice: x: 4, y: 2, z: 16, core: 2. Of those that a mesh axis runs over, the one named last changes fastest.
The devices are a block of a 4x16x16 slice.
Arguments:
- pair_state: bfloat16 [1024, 512, 128], P(('groups', 'row'), ('col', 'ksplit')), parts along dimension 0, may hold values from -6 to 6
- residue_mask: int32 [1024], P('groups'), parts along dimension 0, may hold values 0 or 1
- input_gain: float32 [128], replicated, may hold values from 0.1 to 1.9
- input_shift: float32 [128], replicated, may hold values from -3 to 3
- left_right: bfloat16 [128, 512], replicated, may hold values from -0.5 to 0.5
- output_gate: bfloat16 [128, 128], replicated, may hold values from -0.5 to 0.5
- final_gain: float32 [128], replicated, may hold values from 0.1 to 1.9
- final_shift: float32 [128], replicated, may hold values from -3 to 3
- output_weight: bfloat16 [128, 128], replicated, may hold values from -0.5 to 0.5
Outputs:
- pair_update: bfloat16 [1024, 512, 128], P(('groups', 'row'), ('col', 'ksplit')), parts along dimension 0
The draws below stay inside these ranges and needn't reach their ends.
There are 2 independent parts, one for each index of `groups`. The reference program is written for one: setup_inputs(seed, part) draws one part's arguments, and reference() takes and returns one part's arrays. A program takes and returns all parts, laid end to end along the dimension named above; an argument that names none is the same for every part. Nothing has to cross between parts.
All inputs are finite; a program needn't handle non-finite values.
Results may differ from the reference program's by a relative error of at most 0.0053.
Values may be sent and summed in bfloat16 or wider, within the bound.
No kernel may reach another device: no remote copies, remote signals or barrier semaphores. Data moves between devices by JAX's collectives and lax.ppermute only.
A program may use at most 64 MiB of HBM per device.

```python
import jax
import jax.numpy as jnp
from jax import lax

C = 128
H = 128
N = 512
N_ROW = 16


def plant(entries, rng, smallest, top_value):
    longest = entries.shape.index(max(entries.shape))
    spots = []
    for shift in (0, 1):
        where = [jax.random.randint(jax.random.fold_in(rng, axis), (), 0, length) for axis, length in enumerate(entries.shape)]
        where[longest] = (where[longest] + shift) % entries.shape[longest]
        spots.append(tuple(where))
    return entries.at[spots[0]].set(smallest).at[spots[1]].set(top_value)


def shard_levels(rng, dims, split, smallest, largest):
    level, own = 1.0, jax.random.fold_in(rng, 6)
    for dim, parts in split:
        heights = jnp.exp(jax.random.uniform(jax.random.fold_in(own, dim), (parts,), jnp.float32, smallest / len(split), largest / len(split)))
        level = level * jnp.repeat(heights, dims[dim] // parts).reshape([-1 if axis == dim else 1 for axis in range(len(dims))])
    return level


def scatter_about(own_key, shape, scale, most, pieces=(), held_as=jnp.bfloat16):
    loudness = shard_levels(own_key, shape, pieces, -0.22, 0.18) if pieces else 1.0
    entries = jax.random.normal(own_key, shape, jnp.float32) * scale * loudness
    return jnp.minimum(jnp.maximum(entries, -most), most).astype(held_as)


def setup_inputs(seed: int = 0, part: int = 0) -> dict:
    seeds = jax.random.split(jax.random.key(seed), 10)
    own_keys = jax.random.split(jax.random.fold_in(seeds[9], part), 10)
    return {
        "pair_state": scatter_about(own_keys[0], (N, N, C), 1.0, 6.0, ((0, 16), (1, 8))),
        "residue_mask": plant((jax.random.randint(own_keys[1], (N,), 0, 4) < 3).astype(jnp.int32), jax.random.fold_in(own_keys[1], 1), 0, 1),
        "input_gain": jnp.clip(1.0 + 0.18 * jax.random.normal(seeds[2], (C,), jnp.float32), 0.1, 1.9),
        "input_shift": scatter_about(seeds[3], (C,), 0.5, 3.0, (), jnp.float32),
        "left_right": scatter_about(seeds[4], (C, 4 * H), C ** -0.5, 0.5),
        "output_gate": scatter_about(seeds[5], (C, C), C ** -0.5, 0.5),
        "final_gain": jnp.clip(1.0 + 0.18 * jax.random.normal(seeds[6], (H,), jnp.float32), 0.1, 1.9),
        "final_shift": scatter_about(seeds[7], (H,), 0.5, 3.0, (), jnp.float32),
        "output_weight": scatter_about(seeds[8], (H, C), H ** -0.5, 0.5),
    }


def norm_last(data, norm_gain, norm_shift):
    average = lax.optimization_barrier(jnp.mean(data, axis=-1, keepdims=True))
    centred = data - average
    spread = lax.optimization_barrier(jnp.mean(centred * centred, axis=-1, keepdims=True))
    return centred * lax.rsqrt(spread + 1e-05) * norm_gain + norm_shift

def reference(pair_state, residue_mask, input_gain, input_shift, left_right, output_gate, final_gain, final_shift, output_weight):
    live_rows = residue_mask.astype(jnp.float32)
    block_rows = N // N_ROW
    blocks_state = pair_state.reshape(N_ROW, block_rows, N, C)
    blocks_live = live_rows.reshape(N_ROW, block_rows)

    def one_block(pair):
        state_block, live_block = pair
        normed_block = norm_last(state_block.astype(jnp.float32), input_gain, input_shift).astype(jnp.bfloat16)
        flat_block = normed_block.reshape(block_rows * N, C)
        live_mask = (live_block[:, None] * live_rows[None, :])[:, :, None]
        left_proj = jnp.dot(flat_block, left_right[:, :2 * H], preferred_element_type=jnp.float32).reshape(block_rows, N, 2 * H)
        left_block = (live_mask * jax.nn.sigmoid(left_proj[:, :, H:]) * left_proj[:, :, :H]).astype(jnp.bfloat16)
        right_proj = jnp.dot(flat_block, left_right[:, 2 * H:], preferred_element_type=jnp.float32).reshape(block_rows, N, 2 * H)
        right_block = (live_mask * jax.nn.sigmoid(right_proj[:, :, H:]) * right_proj[:, :, :H]).astype(jnp.bfloat16)
        return (normed_block, left_block, right_block)
    normed_blocks, left_blocks, right_blocks = lax.map(one_block, (blocks_state, blocks_live))
    normed_in = normed_blocks.reshape(N, N, C)
    left_side = left_blocks.reshape(N, N, H)
    right_side = right_blocks.reshape(N, N, H)
    flat_rows = normed_in.reshape(N * N, C)
    left_major = jnp.transpose(left_side, (2, 0, 1))
    right_major = jnp.transpose(right_side, (2, 0, 1))

    def one_channel(pair):
        lhs, rhs = pair
        return jnp.dot(lhs.astype(jnp.float32), rhs.astype(jnp.float32).T, precision=lax.Precision.HIGHEST)
    mixed_all = lax.map(one_channel, (left_major, right_major))
    mixed_last = jnp.transpose(mixed_all, (1, 2, 0))
    normed_out = norm_last(mixed_last, final_gain, final_shift).astype(jnp.bfloat16)
    gate_values = jax.nn.sigmoid(jnp.dot(flat_rows, output_gate, preferred_element_type=jnp.float32))
    projected_out = jnp.dot(normed_out.reshape(N * N, H), output_weight, preferred_element_type=jnp.float32)
    return (gate_values * projected_out).reshape(N, N, C).astype(jnp.bfloat16)
```

```python
import jax
import jax.numpy as jnp
from jax import lax
from jax.sharding import PartitionSpec as P


def norm_over(data, norm_gain, norm_shift, over_axis):
    average = jnp.mean(data, axis=over_axis, keepdims=True)
    centred = data - average
    spread = jnp.mean(centred * centred, axis=over_axis, keepdims=True)
    return centred * lax.rsqrt(spread + 1e-05) * norm_gain + norm_shift


def gated_side(normed_in, weights, live_mask, hidden):
    values = jnp.einsum(
        "ikc,ch->hik", normed_in, weights[:, :hidden], preferred_element_type=jnp.float32
    )
    gates = jnp.einsum(
        "ikc,ch->hik", normed_in, weights[:, hidden:], preferred_element_type=jnp.float32
    )
    return (live_mask * jax.nn.sigmoid(gates) * values).astype(jnp.bfloat16)


def body(
    pair_state,
    residue_mask,
    input_gain,
    input_shift,
    left_right,
    output_gate,
    final_gain,
    final_shift,
    output_weight,
):
    tile_rows, tile_cols, channels = pair_state.shape
    hidden = output_weight.shape[0]
    every = ("row", "col", "ksplit")
    normed_in = norm_over(pair_state.astype(jnp.float32), input_gain, input_shift, 2).astype(
        jnp.bfloat16
    )
    row_start = lax.axis_index("row") * tile_rows
    col_start = lax.axis_index(("col", "ksplit")) * tile_cols
    row_live = lax.dynamic_slice_in_dim(residue_mask, row_start, tile_rows).astype(jnp.float32)
    col_live = lax.dynamic_slice_in_dim(residue_mask, col_start, tile_cols).astype(jnp.float32)
    live_mask = row_live[:, None] * col_live[None, :]
    left_side = gated_side(normed_in, left_right[:, : 2 * hidden], live_mask, hidden)
    right_side = gated_side(normed_in, left_right[:, 2 * hidden :], live_mask, hidden)
    devices_all = lax.axis_size(every)
    row_count = lax.axis_size("row")
    col_count = devices_all // row_count
    per_device = hidden // devices_all
    both = jnp.concatenate(
        [
            left_side.reshape(devices_all, per_device, tile_rows, tile_cols),
            right_side.reshape(devices_all, per_device, tile_rows, tile_cols),
        ],
        axis=1,
    )
    parts = lax.all_to_all(both, every, split_axis=0, concat_axis=0, tiled=True)
    parts = parts.reshape(row_count, col_count, 2 * per_device, tile_rows, tile_cols)
    whole = parts.transpose(2, 0, 3, 1, 4).reshape(
        2, per_device, row_count * tile_rows, col_count * tile_cols
    )
    products = jnp.einsum(
        "cik,cjk->cij", whole[0], whole[1], preferred_element_type=jnp.float32
    ).astype(jnp.bfloat16)
    returned = products.reshape(per_device, row_count, tile_rows, col_count, tile_cols)
    returned = returned.transpose(1, 3, 0, 2, 4).reshape(
        devices_all, per_device, tile_rows, tile_cols
    )
    received = lax.all_to_all(returned, every, split_axis=0, concat_axis=0, tiled=True)
    mixed_tile = received.reshape(hidden, tile_rows, tile_cols).astype(jnp.float32)
    normed_out = norm_over(
        mixed_tile, final_gain[:, None, None], final_shift[:, None, None], 0
    ).astype(jnp.bfloat16)
    projected_out = jnp.einsum(
        "hij,hc->ijc", normed_out, output_weight, preferred_element_type=jnp.float32
    )
    gate_values = jax.nn.sigmoid(
        jnp.einsum("ijc,cd->ijd", normed_in, output_gate, preferred_element_type=jnp.float32)
    )
    return (gate_values * projected_out).astype(jnp.bfloat16)


def solution(mesh):
    whole = P()
    placed = (P(("groups", "row"), ("col", "ksplit"), None), P("groups")) + (whole,) * 7
    return jax.shard_map(
        body,
        mesh=mesh,
        in_specs=placed,
        out_specs=P(("groups", "row"), ("col", "ksplit"), None),
        check_vma=False,
    )
```

```python
import jax, functools
import jax.numpy as jnp
from jax import lax
from jax.experimental import pallas as pl
from jax.experimental.pallas import tpu as pltpu
F32=jnp.float32; BF16=jnp.bfloat16

def prologue_kernel(where_ref, live_ref, cols_ref, x_ref, gain_ref, shift_ref, wl_ref, wr_ref, both_ref, normed_ref):
    rows, cols, chans = x_ref.shape
    half = rows // 2
    hidden = wl_ref.shape[0] // 2
    lanes = 2 * cols
    low = lax.broadcasted_iota(jnp.int32, (1, lanes), 1) < cols
    vec = cols_ref[pl.ds(where_ref[1] // lanes, 1), :]
    turned = pltpu.roll(vec, cols, 1)
    first = (where_ref[1] % lanes) == 0
    col_live = jnp.where(low == first, vec, turned)
    step = 8
    for base in range(0, half, step):
        parts = []
        for start in (base, base + half):
            data = x_ref[start:start + step].astype(F32)
            average = jnp.mean(data, axis=-1, keepdims=True)
            centred = data - average
            spread = jnp.mean(centred * centred, axis=-1, keepdims=True)
            normed = (centred * lax.rsqrt(spread + 1e-05) * gain_ref[...] + shift_ref[...]).astype(BF16)
            normed_ref[start:start + step] = normed
            parts.append(normed)
        top, bottom = parts
        straight = jnp.stack([top, bottom], axis=1).reshape(step * lanes, chans)
        crossed = jnp.stack([bottom, top], axis=1).reshape(step * lanes, chans)
        nt = (((1,), (1,)), ((), ()))
        left = lax.dot_general(wl_ref[...], straight, nt, preferred_element_type=F32)
        right = lax.dot_general(wr_ref[...], crossed, nt, preferred_element_type=F32)
        left = left[:hidden] * jax.nn.sigmoid(left[hidden:])
        right = right[:hidden] * jax.nn.sigmoid(right[hidden:])
        upper, lower = [], []
        for t in range(step):
            m_top = live_ref[where_ref[0] + base + t].astype(F32)
            m_bot = live_ref[where_ref[0] + base + half + t].astype(F32)
            lt = left[:, t * lanes:(t + 1) * lanes] * (jnp.where(low, m_top, m_bot) * col_live)
            rt = right[:, t * lanes:(t + 1) * lanes] * (jnp.where(low, m_bot, m_top) * col_live)
            upper.append(jnp.where(low, lt, rt))
            lower.append(jnp.where(low, rt, lt))
        both_ref[:, base:base + step, :] = jnp.swapaxes(jnp.stack(upper, axis=0), 0, 1).astype(BF16)
        both_ref[:, base + half:base + half + step, :] = jnp.swapaxes(jnp.stack(lower, axis=0), 0, 1).astype(BF16)

def middle_kernel(in_ref, out_ref):
    nrow, ncol, rows, lanes = in_ref.shape
    half = rows // 2
    cols = lanes // 2
    low = lax.broadcasted_iota(jnp.int32, (1, 1, lanes), 2) < cols
    def sides(k):
        a = in_ref[:, k, :half].astype(F32); b = in_ref[:, k, half:].astype(F32)
        ar = pltpu.roll(a, cols, 2); br = pltpu.roll(b, cols, 2)
        lr = jnp.concatenate([a, br], axis=1); rl = jnp.concatenate([ar, b], axis=1)
        return lr, rl
    lefts, rights = [], []
    for k in range(0, ncol, 2):
        lr0, rl0 = sides(k); lr1, rl1 = sides(k + 1)
        lefts.append(jnp.where(low, lr0, rl1).astype(BF16).reshape(nrow * rows, lanes))
        rights.append(jnp.where(low, rl0, lr1).astype(BF16).reshape(nrow * rows, lanes))
    left = jnp.concatenate(lefts, axis=1); right = jnp.concatenate(rights, axis=1)
    product = lax.dot_general(left, right, (((1,), (1,)), ((), ())), preferred_element_type=F32)
    for k in range(0, ncol, 2):
        tile = product[:, k * cols:(k + 2) * cols].reshape(nrow, rows, lanes)
        a = tile[:, :half]; b = tile[:, half:]
        ar = pltpu.roll(a, cols, 2); br = pltpu.roll(b, cols, 2)
        out_ref[:, k] = jnp.where(low, a, br).astype(BF16)
        out_ref[:, k + 1] = jnp.where(low, ar, b).astype(BF16)

def prologue(x, residue_mask, gain, shift, weights, row_start, col_start):
    rows, cols, chans = x.shape
    hidden = weights.shape[1] // 4
    place = jnp.stack([row_start, col_start]).astype(jnp.int32)
    wt = weights.T
    smem = pl.BlockSpec(memory_space=pltpu.SMEM); vmem = pl.BlockSpec(memory_space=pltpu.VMEM)
    return pl.pallas_call(
        prologue_kernel,
        out_shape=(jax.ShapeDtypeStruct((hidden, rows, 2 * cols), BF16), jax.ShapeDtypeStruct((rows, cols, chans), BF16)),
        in_specs=[smem, smem] + [vmem] * 6,
        out_specs=(vmem, vmem),
        name="prologue",
    )(place, residue_mask, residue_mask.astype(F32).reshape(-1, 2 * cols), x, gain.reshape(1, 1, -1), shift.reshape(1, 1, -1), wt[: 2 * hidden], wt[2 * hidden :])

def middle(parts, row_count, col_count):
    n, rows, lanes = parts.shape
    vmem = pl.BlockSpec(memory_space=pltpu.VMEM)
    out = pl.pallas_call(
        middle_kernel,
        out_shape=jax.ShapeDtypeStruct((row_count, col_count, rows // 2, lanes), BF16),
        in_specs=[vmem], out_specs=vmem, name="middle",
    )(parts.reshape(row_count, col_count, rows, lanes))
    return out.reshape(n, rows // 2, lanes)

from jax.sharding import PartitionSpec as P


def body(
    pair_state,
    residue_mask,
    input_gain,
    input_shift,
    left_right,
    output_gate,
    final_gain,
    final_shift,
    output_weight,
):
    tile_rows, tile_cols, channels = pair_state.shape
    hidden = output_weight.shape[0]
    every = ("row", "col", "ksplit")
    row_start = lax.axis_index("row") * tile_rows
    col_start = lax.axis_index(("col", "ksplit")) * tile_cols
    row_count = lax.axis_size("row")
    col_count = lax.axis_size(("col", "ksplit"))
    both, normed_in = prologue(
        pair_state, residue_mask, input_gain, input_shift, left_right, row_start, col_start
    )
    parts = lax.all_to_all(both, every, split_axis=0, concat_axis=0, tiled=True)
    returned = middle(parts, row_count, col_count)
    received = lax.all_to_all(returned, every, split_axis=0, concat_axis=0, tiled=True)
    mixed = received.astype(F32)
    average = jnp.mean(mixed, axis=0, keepdims=True)
    centred = mixed - average
    spread = jnp.mean(centred * centred, axis=0, keepdims=True)
    normed_out = (
        centred * lax.rsqrt(spread + 1e-05) * final_gain[:, None, None]
        + final_shift[:, None, None]
    ).astype(BF16)
    projected_out = jnp.einsum(
        "hrl,hc->rlc", normed_out, output_weight, preferred_element_type=F32
    )
    projected_out = projected_out.reshape(tile_rows // 2, 2, tile_cols, channels)
    projected_out = projected_out.transpose(1, 0, 2, 3).reshape(tile_rows, tile_cols, channels)
    gate_values = jax.nn.sigmoid(
        jnp.einsum("ijc,cd->ijd", normed_in, output_gate, preferred_element_type=F32)
    )
    return (gate_values * projected_out).astype(BF16)


def solution(mesh):
    whole = P()
    placed = (P(("groups", "row"), ("col", "ksplit"), None), P("groups")) + (whole,) * 7
    return jax.shard_map(
        body,
        mesh=mesh,
        in_specs=placed,
        out_specs=P(("groups", "row"), ("col", "ksplit"), None),
        check_vma=False,
    )
```

```python
import jax
import jax.numpy as jnp
from jax import lax
from jax.experimental import pallas as pl
from jax.experimental.pallas import tpu as pltpu
from jax.sharding import PartitionSpec as P

F32 = jnp.float32
BF16 = jnp.bfloat16
ACROSS = (((1,), (1,)), ((), ()))


def norm_rows(data, norm_gain, norm_shift):
    average = jnp.mean(data, axis=-1, keepdims=True)
    centred = data - average
    spread = jnp.mean(centred * centred, axis=-1, keepdims=True)
    return (centred * lax.rsqrt(spread + 1e-05) * norm_gain + norm_shift).astype(BF16)


def prologue_kernel(live_ref, cols_ref, x_ref, gain_ref, shift_ref, weights_ref, both_ref):
    _, step, cols, chans = x_ref.shape
    hidden = weights_ref.shape[1] // 4
    lanes = 2 * cols
    half = step * pl.num_programs(0)
    row_start = lax.axis_index("row") * (2 * half) + pl.program_id(0) * step
    col_index = lax.axis_index("col") * lax.axis_size("ksplit") + lax.axis_index("ksplit")
    low = lax.broadcasted_iota(jnp.int32, (1, lanes), 1) < cols
    pair = cols_ref[pl.ds(col_index // 2, 1), :].astype(F32)
    swapped = pltpu.roll(pair, cols, 1)
    own_low = jnp.where(low, pair, swapped)
    own_high = jnp.where(low, swapped, pair)
    odd = (col_index % 2).astype(F32)
    col_live = own_high * odd + own_low * (1.0 - odd)
    top = norm_rows(x_ref[0].astype(F32), gain_ref[...], shift_ref[...])
    bottom = norm_rows(x_ref[1].astype(F32), gain_ref[...], shift_ref[...])
    straight = jnp.stack([top, bottom], axis=1).reshape(step * lanes, chans)
    crossed = jnp.stack([bottom, top], axis=1).reshape(step * lanes, chans)
    turned = weights_ref[...].T
    left = lax.dot_general(turned[: 2 * hidden], straight, ACROSS, preferred_element_type=F32)
    right = lax.dot_general(turned[2 * hidden :], crossed, ACROSS, preferred_element_type=F32)
    left = left[:hidden] * jax.nn.sigmoid(left[hidden:])
    right = right[:hidden] * jax.nn.sigmoid(right[hidden:])
    upper, lower = [], []
    for t in range(step):
        live_top = live_ref[row_start + t].astype(F32)
        live_bottom = live_ref[row_start + half + t].astype(F32)
        span = slice(t * lanes, (t + 1) * lanes)
        from_left = left[:, span] * (jnp.where(low, live_top, live_bottom) * col_live)
        from_right = right[:, span] * (jnp.where(low, live_bottom, live_top) * col_live)
        upper.append(jnp.where(low, from_left, from_right))
        lower.append(jnp.where(low, from_right, from_left))
    both_ref[:, 0] = jnp.swapaxes(jnp.stack(upper, axis=0), 0, 1).astype(BF16)
    both_ref[:, 1] = jnp.swapaxes(jnp.stack(lower, axis=0), 0, 1).astype(BF16)


def prologue(pair_state, residue_mask, input_gain, input_shift, left_right):
    rows, cols, chans = pair_state.shape
    hidden = left_right.shape[1] // 4
    half = rows // 2
    step = 8
    lanes = 2 * cols
    still = lambda s: (0, 0)
    both = pl.pallas_call(
        prologue_kernel,
        grid=(half // step,),
        out_shape=jax.ShapeDtypeStruct((hidden, 2, half, lanes), BF16),
        in_specs=[
            pl.BlockSpec(memory_space=pltpu.SMEM),
            pl.BlockSpec((residue_mask.shape[0] // lanes, lanes), still),
            pl.BlockSpec((2, step, cols, chans), lambda s: (0, s, 0, 0)),
            pl.BlockSpec((1, chans), still),
            pl.BlockSpec((1, chans), still),
            pl.BlockSpec((chans, 4 * hidden), still),
        ],
        out_specs=pl.BlockSpec((hidden, 2, step, lanes), lambda s: (0, 0, s, 0)),
        name="prologue",
    )(
        residue_mask,
        residue_mask.reshape(-1, lanes),
        pair_state.reshape(2, half, cols, chans),
        input_gain.reshape(1, -1),
        input_shift.reshape(1, -1),
        left_right,
    )
    return both.reshape(hidden, rows, lanes)


def gate_kernel(x_ref, gain_ref, shift_ref, weights_ref, gate_ref):
    _, rows, cols, chans = x_ref.shape
    normed = norm_rows(x_ref[...].astype(F32), gain_ref[...], shift_ref[...])
    raised = jnp.dot(
        normed.reshape(2 * rows * cols, chans), weights_ref[...], preferred_element_type=F32
    )
    gated = jax.nn.sigmoid(raised).reshape(2, rows, cols, chans)
    gate_ref[:, 0] = gated[0]
    gate_ref[:, 1] = gated[1]


def output_gates(pair_state, input_gain, input_shift, output_gate):
    rows, cols, chans = pair_state.shape
    half = rows // 2
    step = 8
    still = lambda s: (0, 0)
    return pl.pallas_call(
        gate_kernel,
        grid=(half // step,),
        out_shape=jax.ShapeDtypeStruct((half, 2, cols, chans), F32),
        in_specs=[
            pl.BlockSpec((2, step, cols, chans), lambda s: (0, s, 0, 0)),
            pl.BlockSpec((1, chans), still),
            pl.BlockSpec((1, chans), still),
            pl.BlockSpec((chans, chans), still),
        ],
        out_specs=pl.BlockSpec((step, 2, cols, chans), lambda s: (s, 0, 0, 0)),
        cost_estimate=pl.CostEstimate(
            flops=2 * rows * cols * chans * chans,
            bytes_accessed=6 * rows * cols * chans,
            transcendentals=rows * cols * chans,
        ),
        name="output_gates",
    )(
        pair_state.reshape(2, half, cols, chans),
        input_gain.reshape(1, -1),
        input_shift.reshape(1, -1),
        output_gate,
    )


def middle_kernel(in_ref, out_ref):
    nrow, ncol, rows, lanes = in_ref.shape
    half = rows // 2
    cols = lanes // 2
    low = lax.broadcasted_iota(jnp.int32, (1, 1, lanes), 2) < cols

    def sides(k):
        top = in_ref[:, k, :half].astype(F32)
        bottom = in_ref[:, k, half:].astype(F32)
        straight = jnp.concatenate([top, pltpu.roll(bottom, cols, 2)], axis=1)
        crossed = jnp.concatenate([pltpu.roll(top, cols, 2), bottom], axis=1)
        return straight, crossed

    lefts, rights = [], []
    for k in range(0, ncol, 2):
        straight, crossed = sides(k)
        straight_next, crossed_next = sides(k + 1)
        left = jnp.where(low, straight, crossed_next).astype(BF16)
        right = jnp.where(low, crossed, straight_next).astype(BF16)
        lefts.append(left.reshape(nrow * rows, lanes))
        rights.append(right.reshape(nrow * rows, lanes))
    product = lax.dot_general(
        jnp.concatenate(lefts, axis=1),
        jnp.concatenate(rights, axis=1),
        ACROSS,
        preferred_element_type=F32,
    )
    for k in range(0, ncol, 2):
        tile = product[:, k * cols : (k + 2) * cols].reshape(nrow, rows, lanes)
        top = tile[:, :half]
        bottom = tile[:, half:]
        out_ref[:, k] = jnp.where(low, top, pltpu.roll(bottom, cols, 2)).astype(BF16)
        out_ref[:, k + 1] = jnp.where(low, pltpu.roll(top, cols, 2), bottom).astype(BF16)


def middle(parts, row_count, col_count):
    count, rows, lanes = parts.shape
    vmem = pl.BlockSpec(memory_space=pltpu.VMEM)
    returned = pl.pallas_call(
        middle_kernel,
        out_shape=jax.ShapeDtypeStruct((row_count, col_count, rows // 2, lanes), BF16),
        in_specs=[vmem],
        out_specs=vmem,
        name="middle",
    )(parts.reshape(row_count, col_count, rows, lanes))
    return returned.reshape(count, rows // 2, lanes)


def body(
    pair_state,
    residue_mask,
    input_gain,
    input_shift,
    left_right,
    output_gate,
    final_gain,
    final_shift,
    output_weight,
):
    tile_rows, tile_cols, channels = pair_state.shape
    every = ("row", "col", "ksplit")
    row_count = lax.axis_size("row")
    col_count = lax.axis_size(("col", "ksplit"))
    both = prologue(pair_state, residue_mask, input_gain, input_shift, left_right)
    gates = output_gates(pair_state, input_gain, input_shift, output_gate)
    parts = lax.all_to_all(both, every, split_axis=0, concat_axis=0, tiled=True)
    returned = middle(parts, row_count, col_count)
    received = lax.all_to_all(returned, every, split_axis=0, concat_axis=0, tiled=True)
    mixed = received.astype(F32)
    average = jnp.mean(mixed, axis=0, keepdims=True)
    centred = mixed - average
    spread = jnp.mean(centred * centred, axis=0, keepdims=True)
    normed_out = (
        centred * lax.rsqrt(spread + 1e-05) * final_gain[:, None, None]
        + final_shift[:, None, None]
    ).astype(BF16)
    projected_out = jnp.einsum(
        "hrl,hc->rlc", normed_out, output_weight, preferred_element_type=F32
    )
    update = gates * projected_out.reshape(tile_rows // 2, 2, tile_cols, channels)
    update = update.transpose(1, 0, 2, 3).astype(BF16)
    return update.reshape(tile_rows, tile_cols, channels)


def solution(mesh):
    whole = P()
    placed = (P(("groups", "row"), ("col", "ksplit"), None), P("groups")) + (whole,) * 7
    return jax.shard_map(
        body,
        mesh=mesh,
        in_specs=placed,
        out_specs=P(("groups", "row"), ("col", "ksplit"), None),
        check_vma=False,
    )
```

```python
import jax
import jax.numpy as jnp
from jax import lax
from jax.experimental import pallas as pl
from jax.experimental.pallas import tpu as pltpu
from jax.sharding import PartitionSpec as P

F32 = jnp.float32
BF16 = jnp.bfloat16
GRANT = 24 << 20
ACROSS = (((1,), (1,)), ((), ()))


def norm_rows(data, norm_gain, norm_shift):
    average = jnp.mean(data, axis=-1, keepdims=True)
    centred = data - average
    spread = jnp.mean(centred * centred, axis=-1, keepdims=True)
    return (centred * lax.rsqrt(spread + 1e-05) * norm_gain + norm_shift).astype(BF16)


def prologue_kernel(live_ref, cols_ref, x_ref, gain_ref, shift_ref, weights_ref, both_ref):
    _, step, cols, chans = x_ref.shape
    hidden = weights_ref.shape[1] // 4
    lanes = 2 * cols
    half = step * pl.num_programs(0)
    row_start = lax.axis_index("row") * (2 * half) + pl.program_id(0) * step
    col_index = lax.axis_index("col") * lax.axis_size("ksplit") + lax.axis_index("ksplit")
    low = lax.broadcasted_iota(jnp.int32, (1, lanes), 1) < cols
    pair = cols_ref[pl.ds(col_index // 2, 1), :].astype(F32)
    swapped = pltpu.roll(pair, cols, 1)
    own_low = jnp.where(low, pair, swapped)
    own_high = jnp.where(low, swapped, pair)
    odd = (col_index % 2).astype(F32)
    col_live = own_high * odd + own_low * (1.0 - odd)
    top = norm_rows(x_ref[0].astype(F32), gain_ref[...], shift_ref[...])
    bottom = norm_rows(x_ref[1].astype(F32), gain_ref[...], shift_ref[...])
    straight = jnp.stack([top, bottom], axis=1).reshape(step * lanes, chans)
    crossed = jnp.stack([bottom, top], axis=1).reshape(step * lanes, chans)
    turned = weights_ref[...].T
    left = lax.dot_general(turned[: 2 * hidden], straight, ACROSS, preferred_element_type=F32)
    right = lax.dot_general(turned[2 * hidden :], crossed, ACROSS, preferred_element_type=F32)
    left = left[:hidden] * jax.nn.sigmoid(left[hidden:])
    right = right[:hidden] * jax.nn.sigmoid(right[hidden:])
    upper, lower = [], []
    for t in range(step):
        live_top = live_ref[row_start + t].astype(F32)
        live_bottom = live_ref[row_start + half + t].astype(F32)
        span = slice(t * lanes, (t + 1) * lanes)
        from_left = left[:, span] * (jnp.where(low, live_top, live_bottom) * col_live)
        from_right = right[:, span] * (jnp.where(low, live_bottom, live_top) * col_live)
        upper.append(jnp.where(low, from_left, from_right))
        lower.append(jnp.where(low, from_right, from_left))
    both_ref[:, 0] = jnp.swapaxes(jnp.stack(upper, axis=0), 0, 1).astype(BF16)
    both_ref[:, 1] = jnp.swapaxes(jnp.stack(lower, axis=0), 0, 1).astype(BF16)


def prologue(pair_state, residue_mask, input_gain, input_shift, left_right):
    rows, cols, chans = pair_state.shape
    hidden = left_right.shape[1] // 4
    half = rows // 2
    step = 8
    lanes = 2 * cols
    still = lambda s: (0, 0)
    both = pl.pallas_call(
        prologue_kernel,
        grid=(half // step,),
        out_shape=jax.ShapeDtypeStruct((hidden, 2, half, lanes), BF16),
        in_specs=[
            pl.BlockSpec(memory_space=pltpu.SMEM),
            pl.BlockSpec((residue_mask.shape[0] // lanes, lanes), still),
            pl.BlockSpec((2, step, cols, chans), lambda s: (0, s, 0, 0)),
            pl.BlockSpec((1, chans), still),
            pl.BlockSpec((1, chans), still),
            pl.BlockSpec((chans, 4 * hidden), still),
        ],
        out_specs=pl.BlockSpec((hidden, 2, step, lanes), lambda s: (0, 0, s, 0)),
        name="prologue",
    )(
        residue_mask,
        residue_mask.reshape(-1, lanes),
        pair_state.reshape(2, half, cols, chans),
        input_gain.reshape(1, -1),
        input_shift.reshape(1, -1),
        left_right,
    )
    return both.reshape(hidden, rows, lanes)


def gate_kernel(
    x_ref, gain_ref, shift_ref, weights_ref, scale_ref, offset_ref, gate_ref, scaled_ref, moved_ref
):
    rows, cols, chans = x_ref.shape
    normed = norm_rows(x_ref[...].astype(F32), gain_ref[...], shift_ref[...])
    raised = jnp.dot(
        normed.reshape(rows * cols, chans), weights_ref[...], preferred_element_type=F32
    )
    gate_ref[...] = jax.nn.sigmoid(raised).reshape(rows, cols, chans)
    scaled_ref[...] = scale_ref[...]
    moved_ref[...] = offset_ref[...]


def output_gates(pair_state, input_gain, input_shift, output_gate, final_gain, final_shift):
    rows, cols, chans = pair_state.shape
    hidden = final_gain.shape[0]
    vmem = pl.BlockSpec(memory_space=pltpu.VMEM)
    return pl.pallas_call(
        gate_kernel,
        out_shape=(
            jax.ShapeDtypeStruct((rows, cols, chans), F32),
            jax.ShapeDtypeStruct((1, hidden), F32),
            jax.ShapeDtypeStruct((1, hidden), F32),
        ),
        in_specs=[vmem] * 6,
        out_specs=(vmem,) * 3,
        cost_estimate=pl.CostEstimate(
            flops=2 * rows * cols * chans * chans,
            bytes_accessed=6 * rows * cols * chans,
            transcendentals=rows * cols * chans,
        ),
        compiler_params=pltpu.CompilerParams(vmem_limit_bytes=GRANT),
        name="output_gates",
    )(
        pair_state,
        input_gain.reshape(1, -1),
        input_shift.reshape(1, -1),
        output_gate,
        final_gain.reshape(1, -1),
        final_shift.reshape(1, -1),
    )


def middle_kernel(in_ref, out_ref, product_ref):
    nrow, ncol, rows, lanes = in_ref.shape
    half = rows // 2
    cols = lanes // 2
    low = lax.broadcasted_iota(jnp.int32, (1, 1, lanes), 2) < cols

    def sides(k):
        top = in_ref[:, k, :half].astype(F32)
        bottom = in_ref[:, k, half:].astype(F32)
        straight = jnp.concatenate([top, pltpu.roll(bottom, cols, 2)], axis=1)
        crossed = jnp.concatenate([pltpu.roll(top, cols, 2), bottom], axis=1)
        return straight, crossed

    lefts, rights = [], []
    for k in range(0, ncol, 2):
        straight, crossed = sides(k)
        straight_next, crossed_next = sides(k + 1)
        left = jnp.where(low, straight, crossed_next).astype(BF16)
        right = jnp.where(low, crossed, straight_next).astype(BF16)
        lefts.append(left.reshape(nrow * rows, lanes))
        rights.append(right.reshape(nrow * rows, lanes))
    product = lax.dot_general(
        jnp.concatenate(lefts, axis=1),
        jnp.concatenate(rights, axis=1),
        ACROSS,
        preferred_element_type=F32,
    )
    for k in range(0, ncol, 2):
        product_ref[k // 2] = product[:, k * cols : (k + 2) * cols]
        even = product_ref[k // 2, pl.ds(0, nrow * half, 2), :].reshape(nrow, half, lanes)
        uneven = product_ref[k // 2, pl.ds(1, nrow * half, 2), :].reshape(nrow, half, lanes)
        out_ref[:, k] = jnp.where(low, even, pltpu.roll(uneven, cols, 2)).astype(BF16)
        out_ref[:, k + 1] = jnp.where(low, pltpu.roll(even, cols, 2), uneven).astype(BF16)


def middle(parts, row_count, col_count):
    count, rows, lanes = parts.shape
    vmem = pl.BlockSpec(memory_space=pltpu.VMEM)
    returned = pl.pallas_call(
        middle_kernel,
        out_shape=jax.ShapeDtypeStruct((row_count, col_count, rows // 2, lanes), BF16),
        in_specs=[vmem],
        out_specs=vmem,
        scratch_shapes=[pltpu.VMEM((col_count // 2, row_count * rows, lanes), F32)],
        compiler_params=pltpu.CompilerParams(vmem_limit_bytes=GRANT),
        name="middle",
    )(parts.reshape(row_count, col_count, rows, lanes))
    return returned.reshape(count, rows // 2, lanes)


def body(
    pair_state,
    residue_mask,
    input_gain,
    input_shift,
    left_right,
    output_gate,
    final_gain,
    final_shift,
    output_weight,
):
    tile_rows, tile_cols, channels = pair_state.shape
    every = ("row", "col", "ksplit")
    row_count = lax.axis_size("row")
    col_count = lax.axis_size(("col", "ksplit"))
    both = prologue(pair_state, residue_mask, input_gain, input_shift, left_right)
    gates, scale, offset = output_gates(
        pair_state, input_gain, input_shift, output_gate, final_gain, final_shift
    )
    parts = lax.all_to_all(both, every, split_axis=0, concat_axis=0, tiled=True)
    returned = middle(parts, row_count, col_count)
    received = lax.all_to_all(returned, every, split_axis=0, concat_axis=0, tiled=True)
    mixed = received.astype(F32)
    average = jnp.mean(mixed, axis=0, keepdims=True)
    centred = mixed - average
    spread = jnp.mean(centred * centred, axis=0, keepdims=True)
    normed_out = (
        centred * lax.rsqrt(spread + 1e-05) * scale.reshape(-1, 1, 1) + offset.reshape(-1, 1, 1)
    ).astype(BF16)
    projected_out = jnp.einsum(
        "hrl,hc->rlc", normed_out, output_weight, preferred_element_type=F32
    )
    return (gates * projected_out.reshape(tile_rows, tile_cols, channels)).astype(BF16)


def solution(mesh):
    whole = P()
    placed = (P(("groups", "row"), ("col", "ksplit"), None), P("groups")) + (whole,) * 7
    return jax.shard_map(
        body,
        mesh=mesh,
        in_specs=placed,
        out_specs=P(("groups", "row"), ("col", "ksplit"), None),
        check_vma=False,
    )
```

```python
import jax
import jax.numpy as jnp
from jax import lax
from jax.experimental import pallas as pl
from jax.experimental.pallas import tpu as pltpu
from jax.sharding import PartitionSpec as P

F32 = jnp.float32
BF16 = jnp.bfloat16
GRANT = 24 << 20
ACROSS = (((1,), (1,)), ((), ()))


def norm_rows(data, norm_gain, norm_shift):
    average = jnp.mean(data, axis=-1, keepdims=True)
    centred = data - average
    spread = jnp.mean(centred * centred, axis=-1, keepdims=True)
    return (centred * lax.rsqrt(spread + 1e-05) * norm_gain + norm_shift).astype(BF16)


def prologue_kernel(live_ref, cols_ref, x_ref, gain_ref, shift_ref, weights_ref, both_ref):
    _, step, cols, chans = x_ref.shape
    hidden = weights_ref.shape[1] // 4
    lanes = 2 * cols
    half = step * pl.num_programs(0)
    row_start = lax.axis_index("row") * (2 * half) + pl.program_id(0) * step
    col_index = lax.axis_index("col") * lax.axis_size("ksplit") + lax.axis_index("ksplit")
    low = lax.broadcasted_iota(jnp.int32, (1, lanes), 1) < cols
    pair = cols_ref[pl.ds(col_index // 2, 1), :].astype(F32)
    swapped = pltpu.roll(pair, cols, 1)
    own_low = jnp.where(low, pair, swapped)
    own_high = jnp.where(low, swapped, pair)
    odd = (col_index % 2).astype(F32)
    col_live = own_high * odd + own_low * (1.0 - odd)
    top = norm_rows(x_ref[0].astype(F32), gain_ref[...], shift_ref[...])
    bottom = norm_rows(x_ref[1].astype(F32), gain_ref[...], shift_ref[...])
    straight = jnp.stack([top, bottom], axis=1).reshape(step * lanes, chans)
    crossed = jnp.stack([bottom, top], axis=1).reshape(step * lanes, chans)
    turned = weights_ref[...].T
    left = lax.dot_general(turned[: 2 * hidden], straight, ACROSS, preferred_element_type=F32)
    right = lax.dot_general(turned[2 * hidden :], crossed, ACROSS, preferred_element_type=F32)
    left = left[:hidden] * jax.nn.sigmoid(left[hidden:])
    right = right[:hidden] * jax.nn.sigmoid(right[hidden:])
    upper, lower = [], []
    for t in range(step):
        live_top = live_ref[row_start + t].astype(F32)
        live_bottom = live_ref[row_start + half + t].astype(F32)
        span = slice(t * lanes, (t + 1) * lanes)
        from_left = left[:, span] * (jnp.where(low, live_top, live_bottom) * col_live)
        from_right = right[:, span] * (jnp.where(low, live_bottom, live_top) * col_live)
        upper.append(jnp.where(low, from_left, from_right))
        lower.append(jnp.where(low, from_right, from_left))
    both_ref[:, 0] = jnp.swapaxes(jnp.stack(upper, axis=0), 0, 1).astype(BF16)
    both_ref[:, 1] = jnp.swapaxes(jnp.stack(lower, axis=0), 0, 1).astype(BF16)


def prologue(pair_state, residue_mask, input_gain, input_shift, left_right):
    rows, cols, chans = pair_state.shape
    hidden = left_right.shape[1] // 4
    half = rows // 2
    step = 8
    lanes = 2 * cols
    still = lambda s: (0, 0)
    both = pl.pallas_call(
        prologue_kernel,
        grid=(half // step,),
        out_shape=jax.ShapeDtypeStruct((hidden, 2, half, lanes), BF16),
        in_specs=[
            pl.BlockSpec(memory_space=pltpu.SMEM),
            pl.BlockSpec((residue_mask.shape[0] // lanes, lanes), still),
            pl.BlockSpec((2, step, cols, chans), lambda s: (0, s, 0, 0)),
            pl.BlockSpec((1, chans), still),
            pl.BlockSpec((1, chans), still),
            pl.BlockSpec((chans, 4 * hidden), still),
        ],
        out_specs=pl.BlockSpec((hidden, 2, step, lanes), lambda s: (0, 0, s, 0)),
        name="prologue",
    )(
        residue_mask,
        residue_mask.reshape(-1, lanes),
        pair_state.reshape(2, half, cols, chans),
        input_gain.reshape(1, -1),
        input_shift.reshape(1, -1),
        left_right,
    )
    return both.reshape(hidden, rows, lanes)


def gate_kernel(
    x_ref, gain_ref, shift_ref, weights_ref, scale_ref, offset_ref, gate_ref, scaled_ref, moved_ref
):
    rows, cols, chans = x_ref.shape
    normed = norm_rows(x_ref[...].astype(F32), gain_ref[...], shift_ref[...])
    raised = jnp.dot(
        normed.reshape(rows * cols, chans), weights_ref[...], preferred_element_type=F32
    )
    gate_ref[...] = jax.nn.sigmoid(raised).reshape(rows, cols, chans)
    scaled_ref[...] = scale_ref[...]
    moved_ref[...] = offset_ref[...]


def output_gates(pair_state, input_gain, input_shift, output_gate, final_gain, final_shift):
    rows, cols, chans = pair_state.shape
    hidden = final_gain.shape[0]
    vmem = pl.BlockSpec(memory_space=pltpu.VMEM)
    return pl.pallas_call(
        gate_kernel,
        out_shape=(
            jax.ShapeDtypeStruct((rows, cols, chans), F32),
            jax.ShapeDtypeStruct((1, hidden), F32),
            jax.ShapeDtypeStruct((1, hidden), F32),
        ),
        in_specs=[vmem] * 6,
        out_specs=(vmem,) * 3,
        cost_estimate=pl.CostEstimate(
            flops=2 * rows * cols * chans * chans,
            bytes_accessed=6 * rows * cols * chans,
            transcendentals=rows * cols * chans,
        ),
        compiler_params=pltpu.CompilerParams(vmem_limit_bytes=GRANT),
        name="output_gates",
    )(
        pair_state,
        input_gain.reshape(1, -1),
        input_shift.reshape(1, -1),
        output_gate,
        final_gain.reshape(1, -1),
        final_shift.reshape(1, -1),
    )


def middle_kernel(in_ref, scale_ref, out_ref, passed_ref, product_ref):
    nrow, ncol, rows, lanes = in_ref.shape
    half = rows // 2
    cols = lanes // 2
    low = lax.broadcasted_iota(jnp.int32, (1, 1, lanes), 2) < cols
    passed_ref[...] = scale_ref[...]

    def sides(k):
        top = in_ref[:, k, :half].astype(F32)
        bottom = in_ref[:, k, half:].astype(F32)
        straight = jnp.concatenate([top, pltpu.roll(bottom, cols, 2)], axis=1)
        crossed = jnp.concatenate([pltpu.roll(top, cols, 2), bottom], axis=1)
        return straight, crossed

    lefts, rights = [], []
    for k in range(0, ncol, 2):
        straight, crossed = sides(k)
        straight_next, crossed_next = sides(k + 1)
        left = jnp.where(low, straight, crossed_next).astype(BF16)
        right = jnp.where(low, crossed, straight_next).astype(BF16)
        lefts.append(left.reshape(nrow * rows, lanes))
        rights.append(right.reshape(nrow * rows, lanes))
    product = lax.dot_general(
        jnp.concatenate(lefts, axis=1),
        jnp.concatenate(rights, axis=1),
        ACROSS,
        preferred_element_type=F32,
    )
    for k in range(0, ncol, 2):
        product_ref[k // 2] = product[:, k * cols : (k + 2) * cols]
        even = product_ref[k // 2, pl.ds(0, nrow * half, 2), :].reshape(nrow, half, lanes)
        uneven = product_ref[k // 2, pl.ds(1, nrow * half, 2), :].reshape(nrow, half, lanes)
        out_ref[:, k] = jnp.where(low, even, pltpu.roll(uneven, cols, 2)).astype(BF16)
        out_ref[:, k + 1] = jnp.where(low, pltpu.roll(even, cols, 2), uneven).astype(BF16)


def middle(parts, scale, row_count, col_count):
    count, rows, lanes = parts.shape
    vmem = pl.BlockSpec(memory_space=pltpu.VMEM)
    returned, passed = pl.pallas_call(
        middle_kernel,
        out_shape=(
            jax.ShapeDtypeStruct((row_count, col_count, rows // 2, lanes), BF16),
            jax.ShapeDtypeStruct(scale.shape, F32),
        ),
        in_specs=[vmem] * 2,
        out_specs=(vmem,) * 2,
        scratch_shapes=[pltpu.VMEM((col_count // 2, row_count * rows, lanes), F32)],
        compiler_params=pltpu.CompilerParams(vmem_limit_bytes=GRANT),
        name="middle",
    )(parts.reshape(row_count, col_count, rows, lanes), scale)
    return returned.reshape(count, rows // 2, lanes), passed


def body(
    pair_state,
    residue_mask,
    input_gain,
    input_shift,
    left_right,
    output_gate,
    final_gain,
    final_shift,
    output_weight,
):
    tile_rows, tile_cols, channels = pair_state.shape
    every = ("row", "col", "ksplit")
    row_count = lax.axis_size("row")
    col_count = lax.axis_size(("col", "ksplit"))
    both = prologue(pair_state, residue_mask, input_gain, input_shift, left_right)
    gates, scale, offset = output_gates(
        pair_state, input_gain, input_shift, output_gate, final_gain, final_shift
    )
    parts = lax.all_to_all(both, every, split_axis=0, concat_axis=0, tiled=True)
    returned, scale = middle(parts, scale, row_count, col_count)
    received = lax.all_to_all(returned, every, split_axis=0, concat_axis=0, tiled=True)
    mixed = received.astype(F32)
    average = jnp.mean(mixed, axis=0, keepdims=True)
    centred = mixed - average
    spread = jnp.mean(centred * centred, axis=0, keepdims=True)
    normed_out = (
        centred * lax.rsqrt(spread + 1e-05) * scale.reshape(-1, 1, 1) + offset.reshape(-1, 1, 1)
    ).astype(BF16)
    projected_out = jnp.einsum(
        "hrl,hc->rlc", normed_out, output_weight, preferred_element_type=F32
    )
    return (gates * projected_out.reshape(tile_rows, tile_cols, channels)).astype(BF16)


def solution(mesh):
    whole = P()
    placed = (P(("groups", "row"), ("col", "ksplit"), None), P("groups")) + (whole,) * 7
    return jax.shard_map(
        body,
        mesh=mesh,
        in_specs=placed,
        out_specs=P(("groups", "row"), ("col", "ksplit"), None),
        check_vma=False,
    )
```

```python
import jax
import jax.numpy as jnp
from jax import lax
from jax.experimental import pallas as pl
from jax.experimental.pallas import tpu as pltpu
from jax.sharding import PartitionSpec as P

F32 = jnp.float32
BF16 = jnp.bfloat16
GRANT = 24 << 20
ACROSS = (((1,), (1,)), ((), ()))


def norm_rows(data, norm_gain, norm_shift):
    average = jnp.mean(data, axis=-1, keepdims=True)
    centred = data - average
    spread = jnp.mean(centred * centred, axis=-1, keepdims=True)
    return (centred * lax.rsqrt(spread + 1e-05) * norm_gain + norm_shift).astype(BF16)


def prologue_kernel(live_ref, cols_ref, x_ref, gain_ref, shift_ref, weights_ref, both_ref):
    _, step, cols, chans = x_ref.shape
    hidden = weights_ref.shape[1] // 4
    lanes = 2 * cols
    half = step * pl.num_programs(0)
    row_start = lax.axis_index("row") * (2 * half) + pl.program_id(0) * step
    col_index = lax.axis_index("col") * lax.axis_size("ksplit") + lax.axis_index("ksplit")
    low = lax.broadcasted_iota(jnp.int32, (1, lanes), 1) < cols
    pair = cols_ref[pl.ds(col_index // 2, 1), :].astype(F32)
    swapped = pltpu.roll(pair, cols, 1)
    own_low = jnp.where(low, pair, swapped)
    own_high = jnp.where(low, swapped, pair)
    odd = (col_index % 2).astype(F32)
    col_live = own_high * odd + own_low * (1.0 - odd)
    top = norm_rows(x_ref[0].astype(F32), gain_ref[...], shift_ref[...])
    bottom = norm_rows(x_ref[1].astype(F32), gain_ref[...], shift_ref[...])
    straight = jnp.stack([top, bottom], axis=1).reshape(step * lanes, chans)
    crossed = jnp.stack([bottom, top], axis=1).reshape(step * lanes, chans)
    turned = weights_ref[...].T
    left = lax.dot_general(turned[: 2 * hidden], straight, ACROSS, preferred_element_type=F32)
    right = lax.dot_general(turned[2 * hidden :], crossed, ACROSS, preferred_element_type=F32)
    left = left[:hidden] * jax.nn.sigmoid(left[hidden:])
    right = right[:hidden] * jax.nn.sigmoid(right[hidden:])
    upper, lower = [], []
    for t in range(step):
        live_top = live_ref[row_start + t].astype(F32)
        live_bottom = live_ref[row_start + half + t].astype(F32)
        span = slice(t * lanes, (t + 1) * lanes)
        from_left = left[:, span] * (jnp.where(low, live_top, live_bottom) * col_live)
        from_right = right[:, span] * (jnp.where(low, live_bottom, live_top) * col_live)
        upper.append(jnp.where(low, from_left, from_right))
        lower.append(jnp.where(low, from_right, from_left))
    both_ref[:, 0] = jnp.swapaxes(jnp.stack(upper, axis=0), 0, 1).astype(BF16)
    both_ref[:, 1] = jnp.swapaxes(jnp.stack(lower, axis=0), 0, 1).astype(BF16)


def prologue(pair_state, residue_mask, input_gain, input_shift, left_right):
    rows, cols, chans = pair_state.shape
    hidden = left_right.shape[1] // 4
    half = rows // 2
    step = 8
    lanes = 2 * cols
    still = lambda s: (0, 0)
    both = pl.pallas_call(
        prologue_kernel,
        grid=(half // step,),
        out_shape=jax.ShapeDtypeStruct((hidden, 2, half, lanes), BF16),
        in_specs=[
            pl.BlockSpec(memory_space=pltpu.SMEM),
            pl.BlockSpec((residue_mask.shape[0] // lanes, lanes), still),
            pl.BlockSpec((2, step, cols, chans), lambda s: (0, s, 0, 0)),
            pl.BlockSpec((1, chans), still),
            pl.BlockSpec((1, chans), still),
            pl.BlockSpec((chans, 4 * hidden), still),
        ],
        out_specs=pl.BlockSpec((hidden, 2, step, lanes), lambda s: (0, 0, s, 0)),
        name="prologue",
    )(
        residue_mask,
        residue_mask.reshape(-1, lanes),
        pair_state.reshape(2, half, cols, chans),
        input_gain.reshape(1, -1),
        input_shift.reshape(1, -1),
        left_right,
    )
    return both.reshape(hidden, rows, lanes)


def gate_kernel(
    x_ref, gain_ref, shift_ref, weights_ref, scale_ref, offset_ref, gate_ref, scaled_ref, moved_ref
):
    rows, cols, chans = x_ref.shape
    normed = norm_rows(x_ref[...].astype(F32), gain_ref[...], shift_ref[...])
    raised = jnp.dot(
        normed.reshape(rows * cols, chans), weights_ref[...], preferred_element_type=F32
    )
    gate_ref[...] = jax.nn.sigmoid(raised).reshape(gate_ref.shape)
    scaled_ref[...] = scale_ref[...]
    moved_ref[...] = offset_ref[...]


def output_gates(pair_state, input_gain, input_shift, output_gate, final_gain, final_shift):
    rows, cols, chans = pair_state.shape
    hidden = final_gain.shape[0]
    vmem = pl.BlockSpec(memory_space=pltpu.VMEM)
    return pl.pallas_call(
        gate_kernel,
        out_shape=(
            jax.ShapeDtypeStruct((rows // 2, 2 * cols, chans), F32),
            jax.ShapeDtypeStruct((1, hidden), F32),
            jax.ShapeDtypeStruct((1, hidden), F32),
        ),
        in_specs=[vmem] * 6,
        out_specs=(vmem,) * 3,
        cost_estimate=pl.CostEstimate(
            flops=2 * rows * cols * chans * chans,
            bytes_accessed=6 * rows * cols * chans,
            transcendentals=rows * cols * chans,
        ),
        compiler_params=pltpu.CompilerParams(vmem_limit_bytes=GRANT),
        name="output_gates",
    )(
        pair_state,
        input_gain.reshape(1, -1),
        input_shift.reshape(1, -1),
        output_gate,
        final_gain.reshape(1, -1),
        final_shift.reshape(1, -1),
    )


def middle_kernel(in_ref, scale_ref, out_ref, passed_ref, product_ref):
    nrow, ncol, rows, lanes = in_ref.shape
    half = rows // 2
    cols = lanes // 2
    low = lax.broadcasted_iota(jnp.int32, (1, 1, lanes), 2) < cols
    passed_ref[...] = scale_ref[...]

    def sides(k):
        top = in_ref[:, k, :half].astype(F32)
        bottom = in_ref[:, k, half:].astype(F32)
        straight = jnp.concatenate([top, pltpu.roll(bottom, cols, 2)], axis=1)
        crossed = jnp.concatenate([pltpu.roll(top, cols, 2), bottom], axis=1)
        return straight, crossed

    lefts, rights = [], []
    for k in range(0, ncol, 2):
        straight, crossed = sides(k)
        straight_next, crossed_next = sides(k + 1)
        left = jnp.where(low, straight, crossed_next).astype(BF16)
        right = jnp.where(low, crossed, straight_next).astype(BF16)
        lefts.append(left.reshape(nrow * rows, lanes))
        rights.append(right.reshape(nrow * rows, lanes))
    product = lax.dot_general(
        jnp.concatenate(lefts, axis=1),
        jnp.concatenate(rights, axis=1),
        ACROSS,
        preferred_element_type=F32,
    )
    for k in range(0, ncol, 2):
        product_ref[k // 2] = product[:, k * cols : (k + 2) * cols]
        even = product_ref[k // 2, pl.ds(0, nrow * half, 2), :].reshape(nrow, half, lanes)
        uneven = product_ref[k // 2, pl.ds(1, nrow * half, 2), :].reshape(nrow, half, lanes)
        out_ref[:, k] = jnp.where(low, even, pltpu.roll(uneven, cols, 2)).astype(BF16)
        out_ref[:, k + 1] = jnp.where(low, pltpu.roll(even, cols, 2), uneven).astype(BF16)


def middle(parts, scale, row_count, col_count):
    count, rows, lanes = parts.shape
    vmem = pl.BlockSpec(memory_space=pltpu.VMEM)
    returned, passed = pl.pallas_call(
        middle_kernel,
        out_shape=(
            jax.ShapeDtypeStruct((row_count, col_count, rows // 2, lanes), BF16),
            jax.ShapeDtypeStruct(scale.shape, F32),
        ),
        in_specs=[vmem] * 2,
        out_specs=(vmem,) * 2,
        scratch_shapes=[pltpu.VMEM((col_count // 2, row_count * rows, lanes), F32)],
        compiler_params=pltpu.CompilerParams(vmem_limit_bytes=GRANT),
        name="middle",
    )(parts.reshape(row_count, col_count, rows, lanes), scale)
    return returned.reshape(count, rows // 2, lanes), passed


def body(
    pair_state,
    residue_mask,
    input_gain,
    input_shift,
    left_right,
    output_gate,
    final_gain,
    final_shift,
    output_weight,
):
    tile_rows, tile_cols, channels = pair_state.shape
    every = ("row", "col", "ksplit")
    row_count = lax.axis_size("row")
    col_count = lax.axis_size(("col", "ksplit"))
    both = prologue(pair_state, residue_mask, input_gain, input_shift, left_right)
    gates, scale, offset = output_gates(
        pair_state, input_gain, input_shift, output_gate, final_gain, final_shift
    )
    parts = lax.all_to_all(both, every, split_axis=0, concat_axis=0, tiled=True)
    returned, scale = middle(parts, scale, row_count, col_count)
    received = lax.all_to_all(returned, every, split_axis=0, concat_axis=0, tiled=True)
    mixed = received.astype(F32)
    average = jnp.mean(mixed, axis=0, keepdims=True)
    centred = mixed - average
    spread = jnp.mean(centred * centred, axis=0, keepdims=True)
    normed_out = (
        centred * lax.rsqrt(spread + 1e-05) * scale.reshape(-1, 1, 1) + offset.reshape(-1, 1, 1)
    ).astype(BF16)
    projected_out = jnp.einsum(
        "hrl,hc->rlc", normed_out, output_weight, preferred_element_type=F32
    )
    update = (gates.reshape(projected_out.shape) * projected_out).astype(BF16)
    return update.reshape(tile_rows, tile_cols, channels)


def solution(mesh):
    whole = P()
    placed = (P(("groups", "row"), ("col", "ksplit"), None), P("groups")) + (whole,) * 7
    return jax.shard_map(
        body,
        mesh=mesh,
        in_specs=placed,
        out_specs=P(("groups", "row"), ("col", "ksplit"), None),
        check_vma=False,
    )
```

```python
import jax
import jax.numpy as jnp
from jax import lax
from jax.experimental import pallas as pl
from jax.experimental.pallas import tpu as pltpu
from jax.sharding import PartitionSpec as P

F32 = jnp.float32
BF16 = jnp.bfloat16
GRANT = 24 << 20
ACROSS = (((1,), (1,)), ((), ()))


def norm_rows(data, norm_gain, norm_shift):
    average = jnp.mean(data, axis=-1, keepdims=True)
    centred = data - average
    spread = jnp.mean(centred * centred, axis=-1, keepdims=True)
    return (centred * lax.rsqrt(spread + 1e-05) * norm_gain + norm_shift).astype(BF16)


def prologue_kernel(
    live_ref, cols_ref, x_ref, gain_ref, shift_ref, weights_ref, both_ref, turned_ref, normed_ref
):
    rows, cols, chans = x_ref.shape
    hidden = weights_ref.shape[1] // 4
    block = both_ref.shape[0]
    lanes = 2 * cols
    half = rows // 2
    step = 8
    nth = pl.program_id(0)

    @pl.when(nth == 0)
    def _():
        turned_ref[...] = weights_ref[...].T
        for start in range(0, rows, step):
            data = x_ref[start : start + step].astype(F32)
            normed_ref[start : start + step] = norm_rows(data, gain_ref[...], shift_ref[...])

    row_start = lax.axis_index("row") * rows
    col_index = lax.axis_index("col") * lax.axis_size("ksplit") + lax.axis_index("ksplit")
    low = lax.broadcasted_iota(jnp.int32, (1, lanes), 1) < cols
    pair = cols_ref[pl.ds(col_index // 2, 1), :].astype(F32)
    swapped = pltpu.roll(pair, cols, 1)
    odd = (col_index % 2).astype(F32)
    col_live = jnp.where(low, swapped, pair) * odd + jnp.where(low, pair, swapped) * (1.0 - odd)
    own = [
        turned_ref[pl.ds(pl.multiple_of(part * hidden + nth * block, block), block), :]
        for part in range(4)
    ]
    left_weights = jnp.concatenate(own[:2], axis=0)
    right_weights = jnp.concatenate(own[2:], axis=0)
    for base in range(0, half, step):
        top = normed_ref[base : base + step]
        bottom = normed_ref[half + base : half + base + step]
        straight = jnp.stack([top, bottom], axis=1).reshape(step * lanes, chans)
        crossed = jnp.stack([bottom, top], axis=1).reshape(step * lanes, chans)
        left = lax.dot_general(left_weights, straight, ACROSS, preferred_element_type=F32)
        right = lax.dot_general(right_weights, crossed, ACROSS, preferred_element_type=F32)
        left = left[:block] * jax.nn.sigmoid(left[block:])
        right = right[:block] * jax.nn.sigmoid(right[block:])
        upper, lower = [], []
        for t in range(step):
            live_top = live_ref[row_start + base + t].astype(F32)
            live_bottom = live_ref[row_start + half + base + t].astype(F32)
            span = slice(t * lanes, (t + 1) * lanes)
            from_left = left[:, span] * (jnp.where(low, live_top, live_bottom) * col_live)
            from_right = right[:, span] * (jnp.where(low, live_bottom, live_top) * col_live)
            upper.append(jnp.where(low, from_left, from_right))
            lower.append(jnp.where(low, from_right, from_left))
        both_ref[:, base : base + step] = jnp.swapaxes(jnp.stack(upper), 0, 1).astype(BF16)
        both_ref[:, half + base : half + base + step] = jnp.swapaxes(
            jnp.stack(lower), 0, 1
        ).astype(BF16)


def prologue(pair_state, residue_mask, input_gain, input_shift, left_right):
    rows, cols, chans = pair_state.shape
    hidden = left_right.shape[1] // 4
    lanes = 2 * cols
    block = hidden // 2
    still = lambda s: (0, 0)
    return pl.pallas_call(
        prologue_kernel,
        grid=(hidden // block,),
        out_shape=jax.ShapeDtypeStruct((hidden, rows, lanes), BF16),
        in_specs=[
            pl.BlockSpec(memory_space=pltpu.SMEM),
            pl.BlockSpec((residue_mask.shape[0] // lanes, lanes), still),
            pl.BlockSpec((rows, cols, chans), lambda s: (0, 0, 0)),
            pl.BlockSpec((1, chans), still),
            pl.BlockSpec((1, chans), still),
            pl.BlockSpec((chans, 4 * hidden), still),
        ],
        out_specs=pl.BlockSpec((block, rows, lanes), lambda s: (s, 0, 0)),
        scratch_shapes=[
            pltpu.VMEM((4 * hidden, chans), BF16),
            pltpu.VMEM((rows, cols, chans), BF16),
        ],
        name="prologue",
    )(
        residue_mask,
        residue_mask.reshape(-1, lanes),
        pair_state,
        input_gain.reshape(1, -1),
        input_shift.reshape(1, -1),
        left_right,
    )


def gate_kernel(
    x_ref, gain_ref, shift_ref, weights_ref, scale_ref, offset_ref, gate_ref, scaled_ref, moved_ref
):
    rows, cols, chans = x_ref.shape
    normed = norm_rows(x_ref[...].astype(F32), gain_ref[...], shift_ref[...])
    raised = jnp.dot(
        normed.reshape(rows * cols, chans), weights_ref[...], preferred_element_type=F32
    )
    gate_ref[...] = jax.nn.sigmoid(raised).reshape(gate_ref.shape)
    scaled_ref[...] = scale_ref[...]
    moved_ref[...] = offset_ref[...]


def output_gates(pair_state, input_gain, input_shift, output_gate, final_gain, final_shift):
    rows, cols, chans = pair_state.shape
    hidden = final_gain.shape[0]
    vmem = pl.BlockSpec(memory_space=pltpu.VMEM)
    return pl.pallas_call(
        gate_kernel,
        out_shape=(
            jax.ShapeDtypeStruct((rows // 2, 2 * cols, chans), F32),
            jax.ShapeDtypeStruct((1, hidden), F32),
            jax.ShapeDtypeStruct((1, hidden), F32),
        ),
        in_specs=[vmem] * 6,
        out_specs=(vmem,) * 3,
        cost_estimate=pl.CostEstimate(
            flops=2 * rows * cols * chans * chans,
            bytes_accessed=6 * rows * cols * chans,
            transcendentals=rows * cols * chans,
        ),
        compiler_params=pltpu.CompilerParams(vmem_limit_bytes=GRANT),
        name="output_gates",
    )(
        pair_state,
        input_gain.reshape(1, -1),
        input_shift.reshape(1, -1),
        output_gate,
        final_gain.reshape(1, -1),
        final_shift.reshape(1, -1),
    )


def middle_kernel(in_ref, scale_ref, out_ref, passed_ref, product_ref):
    nrow, ncol, rows, lanes = in_ref.shape
    half = rows // 2
    cols = lanes // 2
    low = lax.broadcasted_iota(jnp.int32, (1, 1, lanes), 2) < cols
    passed_ref[...] = scale_ref[...]

    def sides(k):
        top = in_ref[:, k, :half].astype(F32)
        bottom = in_ref[:, k, half:].astype(F32)
        straight = jnp.concatenate([top, pltpu.roll(bottom, cols, 2)], axis=1)
        crossed = jnp.concatenate([pltpu.roll(top, cols, 2), bottom], axis=1)
        return straight, crossed

    lefts, rights = [], []
    for k in range(0, ncol, 2):
        straight, crossed = sides(k)
        straight_next, crossed_next = sides(k + 1)
        left = jnp.where(low, straight, crossed_next).astype(BF16)
        right = jnp.where(low, crossed, straight_next).astype(BF16)
        lefts.append(left.reshape(nrow * rows, lanes))
        rights.append(right.reshape(nrow * rows, lanes))
    product = lax.dot_general(
        jnp.concatenate(lefts, axis=1),
        jnp.concatenate(rights, axis=1),
        ACROSS,
        preferred_element_type=F32,
    )
    for k in range(0, ncol, 2):
        product_ref[k // 2] = product[:, k * cols : (k + 2) * cols]
        even = product_ref[k // 2, pl.ds(0, nrow * half, 2), :].reshape(nrow, half, lanes)
        uneven = product_ref[k // 2, pl.ds(1, nrow * half, 2), :].reshape(nrow, half, lanes)
        out_ref[:, k] = jnp.where(low, even, pltpu.roll(uneven, cols, 2)).astype(BF16)
        out_ref[:, k + 1] = jnp.where(low, pltpu.roll(even, cols, 2), uneven).astype(BF16)


def middle(parts, scale, row_count, col_count):
    count, rows, lanes = parts.shape
    vmem = pl.BlockSpec(memory_space=pltpu.VMEM)
    returned, passed = pl.pallas_call(
        middle_kernel,
        out_shape=(
            jax.ShapeDtypeStruct((row_count, col_count, rows // 2, lanes), BF16),
            jax.ShapeDtypeStruct(scale.shape, F32),
        ),
        in_specs=[vmem] * 2,
        out_specs=(vmem,) * 2,
        scratch_shapes=[pltpu.VMEM((col_count // 2, row_count * rows, lanes), F32)],
        compiler_params=pltpu.CompilerParams(vmem_limit_bytes=GRANT),
        name="middle",
    )(parts.reshape(row_count, col_count, rows, lanes), scale)
    return returned.reshape(count, rows // 2, lanes), passed


def body(
    pair_state,
    residue_mask,
    input_gain,
    input_shift,
    left_right,
    output_gate,
    final_gain,
    final_shift,
    output_weight,
):
    tile_rows, tile_cols, channels = pair_state.shape
    every = ("row", "col", "ksplit")
    row_count = lax.axis_size("row")
    col_count = lax.axis_size(("col", "ksplit"))
    both = prologue(pair_state, residue_mask, input_gain, input_shift, left_right)
    gates, scale, offset = output_gates(
        pair_state, input_gain, input_shift, output_gate, final_gain, final_shift
    )
    parts = lax.all_to_all(both, every, split_axis=0, concat_axis=0, tiled=True)
    returned, scale = middle(parts, scale, row_count, col_count)
    received = lax.all_to_all(returned, every, split_axis=0, concat_axis=0, tiled=True)
    mixed = received.astype(F32)
    average = jnp.mean(mixed, axis=0, keepdims=True)
    centred = mixed - average
    spread = jnp.mean(centred * centred, axis=0, keepdims=True)
    normed_out = (
        centred * lax.rsqrt(spread + 1e-05) * scale.reshape(-1, 1, 1) + offset.reshape(-1, 1, 1)
    ).astype(BF16)
    projected_out = jnp.einsum(
        "hrl,hc->rlc", normed_out, output_weight, preferred_element_type=F32
    )
    update = (gates.reshape(projected_out.shape) * projected_out).astype(BF16)
    return update.reshape(tile_rows, tile_cols, channels)


def solution(mesh):
    whole = P()
    placed = (P(("groups", "row"), ("col", "ksplit"), None), P("groups")) + (whole,) * 7
    return jax.shard_map(
        body,
        mesh=mesh,
        in_specs=placed,
        out_specs=P(("groups", "row"), ("col", "ksplit"), None),
        check_vma=False,
    )
```
